32 devices in a mesh: group: 4 (over z), dom: 8 (over y, x, core).
Axes of the slice: x: 2, y: 2, z: 4, core: 2. Of those that a mesh axis runs over, the one named last changes fastest.
Arguments:
- features: bfloat16 [16384, 128], P(('group', 'dom')), may hold values from -6 to 6
- cotangent: bfloat16 [16384, 128], P(('group', 'dom')), may hold values from -6 to 6
- fine_send: int32 [256, 16], P(('group', 'dom')), may hold values from 0 to 512, as said below
- fine_rim: int32 [64, 128], P(('group', 'dom')), may hold values from 0 to 511
- fine_src: int32 [131072], P(('group', 'dom')), may hold values from 0 to 895, as said below
- fine_dst: int32 [131072], P(('group', 'dom')), may hold values from 0 to 511
- fine_pool: int32 [16384], P(('group', 'dom')), may hold values from 0 to 255, as said below
- coarse_send: int32 [256, 4], P(('group', 'dom')), may hold values from 0 to 32, as said below
- coarse_src: int32 [8192], P(('group', 'dom')), may hold values from 0 to 63, as said below
- coarse_dst: int32 [8192], P(('group', 'dom')), may hold values from 0 to 31
- coarse_pool: int32 [1024], P(('group', 'dom')), may hold values from 0 to 511
- w_send: bfloat16 [128, 128], replicated, may hold values from -0.5 to 0.5
- w_recv: bfloat16 [128, 128], replicated, may hold values from -0.5 to 0.5
- w_node: bfloat16 [128, 128], replicated, may hold values from -0.5 to 0.5
- v_send: bfloat16 [128, 128], replicated, may hold values from -0.5 to 0.5
- v_recv: bfloat16 [128, 128], replicated, may hold values from -0.5 to 0.5
- v_node: bfloat16 [128, 128], replicated, may hold values from -0.5 to 0.5
- w_top: bfloat16 [128, 128], replicated, may hold values from -0.5 to 0.5
Outputs:
- flow: bfloat16 [16384, 128], P(('group', 'dom'))
- grad_features: float32 [16384, 128], P(('group', 'dom'))
- grad_send: float32 [128, 128], replicated
The draws below stay inside these ranges and needn't reach their ends.
Inputs may be any that keep to these rules, and one draw needn't show every extreme that they name: `fine_send`: each device holds 8 rows of 16: row p lists own node rows for the device with dom index p of its group; the value 512 marks an empty slot, live slots come first, and three rows of every device are full. `fine_rim`: each device holds two rows: the first go to the previous group's device of the same dom index, the second to the next group's. `fine_src`: index into the device's extended rows: its 512 nodes, 128 rows from its group in dom order, 128 rows from the previous group, 128 from the next. `fine_pool`: coarse node numbered within the node's group. `coarse_send`: as fine_send with 4 slots a row and 32 marking an empty slot. `coarse_src`: index into the device's coarse rows, then 8 * 4 rows from its group in dom order.
All inputs are finite; a program needn't handle non-finite values.
Results may differ from the reference program's by a relative error of at most 0.025.
Values may be sent and summed in bfloat16 or wider, within the bound.
No kernel may reach another device: no remote copies, remote signals or barrier semaphores. Data moves between devices by JAX's collectives and lax.ppermute only.
A program may use at most 64 MiB of HBM per device.

```python
import jax
import jax.numpy as jnp
from jax import lax

H = 128
NODE_DEV = 512
EDGE_DEV = 4096
NC_DEV = 32
CEDGE_DEV = 256
SLOT = 16
SLOT_G = 128
CSLOT = 4
NCC = 512
NODES = 16384
N_GROUP = 4
N_DOM = 8


def halo_lists(key, slots, blank_row):
    blocks = N_GROUP * N_DOM * N_DOM
    rows = jax.random.randint(jax.random.fold_in(key, 11), (blocks, slots), 0, blank_row)
    counts = jax.random.randint(jax.random.fold_in(key, 12), (blocks, 1), 1, slots + 1)
    order = jnp.arange(blocks, dtype=jnp.int32)
    device = order // N_DOM
    dom_index = device % N_DOM
    peer = order % N_DOM
    opposite = (dom_index + N_DOM // 2) % N_DOM
    after = (dom_index + 1) % N_DOM
    before = (dom_index + N_DOM - 1) % N_DOM
    full = (peer == opposite) | (peer == after) | (peer == before)
    counts = jnp.where(full[:, None], slots, counts)
    live = jnp.arange(slots, dtype=jnp.int32)[None, :] < counts
    return jnp.where(live, rows, blank_row).astype(jnp.int32)


def edge_sources(key, total, per_device, local_rows, extra_rows, slots):
    near = jax.random.randint(jax.random.fold_in(key, 21), (total,), 0, local_rows)
    far = jax.random.randint(jax.random.fold_in(key, 22), (total,), local_rows, local_rows + extra_rows)
    choose = jax.random.randint(jax.random.fold_in(key, 23), (total,), 0, 8)
    order = jnp.arange(total, dtype=jnp.int32)
    dom_index = order // per_device % N_DOM
    opposite = (dom_index + N_DOM // 2) % N_DOM
    within = jax.random.randint(jax.random.fold_in(key, 24), (total,), 0, slots)
    across = local_rows + opposite * slots + within
    picked = jnp.where(choose < 2, far, jnp.where(choose == 2, across, near))
    return picked.astype(jnp.int32)


def draw_fine_send(key, part):
    return halo_lists(key, SLOT, NODE_DEV)


def draw_coarse_send(key, part):
    return halo_lists(key, CSLOT, NC_DEV)


def draw_fine_src(key, part):
    return edge_sources(key, N_GROUP * N_DOM * EDGE_DEV, EDGE_DEV, NODE_DEV, N_DOM * SLOT + 2 * SLOT_G, SLOT)


def draw_coarse_src(key, part):
    return edge_sources(key, N_GROUP * N_DOM * CEDGE_DEV, CEDGE_DEV, NC_DEV, N_DOM * CSLOT, CSLOT)


def draw_fine_pool(key, part):
    total = N_GROUP * N_DOM * NODE_DEV
    order = jnp.arange(total, dtype=jnp.int32)
    dom_index = order // NODE_DEV % N_DOM
    near = dom_index * NC_DEV + jax.random.randint(jax.random.fold_in(key, 31), (total,), 0, NC_DEV)
    far = jax.random.randint(jax.random.fold_in(key, 32), (total,), 0, NC_DEV * N_DOM)
    choose = jax.random.randint(jax.random.fold_in(key, 33), (total,), 0, 4)
    return jnp.where(choose == 0, far, near).astype(jnp.int32)


def with_ends(array, own_key, least, top_value):
    shape = array.shape
    index_at = [jax.random.randint(jax.random.fold_in(own_key, axis), (), 0, shape[axis]) for axis in range(len(shape))]
    array = array.at[tuple(index_at)].set(least)
    longest = shape.index(max(shape))
    index_at[longest] = (index_at[longest] + 1) % shape[longest]
    return array.at[tuple(index_at)].set(top_value)


def steps_of(stream_key, dims, cuts, low, high):
    factor_of, own = 1.0, jax.random.fold_in(stream_key, 6)
    for position, shards_of in cuts:
        steps = jnp.exp(jax.random.uniform(jax.random.fold_in(own, position), (shards_of,), jnp.float32, low / len(cuts), high / len(cuts)))
        factor_of = factor_of * jnp.repeat(steps, dims[position] // shards_of).reshape([-1 if axis == position else 1 for axis in range(len(dims))])
    return factor_of


def scatter_about(own_key, shape, scale, reach, cuts=(), kind=jnp.bfloat16):
    entries = scale * jax.random.normal(own_key, shape, jnp.float32)
    if cuts:
        entries = entries * steps_of(own_key, shape, cuts, -0.22, 0.18)
    return jnp.clip(entries, -reach, reach).astype(kind)


def setup_inputs(seed: int = 0) -> dict:
    key_list = jax.random.split(jax.random.key(seed), 19)
    features = scatter_about(key_list[0], (NODES, H), 1.0, 6.0, ((0, 32),))
    cotangent = scatter_about(key_list[1], (NODES, H), 1.0, 6.0, ((0, 32),))
    fine_send = draw_fine_send(jax.random.fold_in(key_list[18], 71), 0)
    fine_rim = with_ends(jax.random.randint(key_list[3], (N_GROUP * N_DOM * 2, SLOT_G), 0, NODE_DEV), jax.random.fold_in(key_list[3], 1), 0, NODE_DEV - 1).astype(jnp.int32)
    fine_src = draw_fine_src(jax.random.fold_in(key_list[18], 71), 0)
    fine_dst = with_ends(jax.random.randint(key_list[5], (N_GROUP * N_DOM * EDGE_DEV,), 0, NODE_DEV), jax.random.fold_in(key_list[5], 1), 0, NODE_DEV - 1).astype(jnp.int32)
    fine_pool = draw_fine_pool(jax.random.fold_in(key_list[18], 71), 0)
    coarse_send = draw_coarse_send(jax.random.fold_in(key_list[18], 71), 0)
    coarse_src = draw_coarse_src(jax.random.fold_in(key_list[18], 71), 0)
    coarse_dst = with_ends(jax.random.randint(key_list[9], (N_GROUP * N_DOM * CEDGE_DEV,), 0, NC_DEV), jax.random.fold_in(key_list[9], 1), 0, NC_DEV - 1).astype(jnp.int32)
    coarse_pool = with_ends(jax.random.randint(key_list[10], (N_GROUP * N_DOM * NC_DEV,), 0, NCC), jax.random.fold_in(key_list[10], 1), 0, NCC - 1).astype(jnp.int32)
    w_send = scatter_about(key_list[11], (H, H), H ** -0.5, 0.5)
    w_recv = scatter_about(key_list[12], (H, H), H ** -0.5, 0.5)
    w_node = scatter_about(key_list[13], (H, H), H ** -0.5, 0.5)
    v_send = scatter_about(key_list[14], (H, H), H ** -0.5, 0.5)
    v_recv = scatter_about(key_list[15], (H, H), H ** -0.5, 0.5)
    v_node = scatter_about(key_list[16], (H, H), H ** -0.5, 0.5)
    w_top = scatter_about(key_list[17], (H, H), H ** -0.5, 0.5)
    return dict(features=features, cotangent=cotangent, fine_send=fine_send, fine_rim=fine_rim, fine_src=fine_src, fine_dst=fine_dst, fine_pool=fine_pool, coarse_send=coarse_send, coarse_src=coarse_src, coarse_dst=coarse_dst, coarse_pool=coarse_pool, w_send=w_send, w_recv=w_recv, w_node=w_node, v_send=v_send, v_recv=v_recv, v_node=v_node, w_top=w_top)


def silu_slope(values):
    sigma = jax.nn.sigmoid(values)
    return sigma * (1.0 + values * (1.0 - sigma))


def edge_forward(extended, own_rows, sources, targets, w_send, w_recv, w_node):
    preact = jnp.dot(extended[sources], w_send, preferred_element_type=jnp.float32)
    preact = preact + jnp.dot(own_rows[targets], w_recv, preferred_element_type=jnp.float32)
    message = jax.nn.silu(preact).astype(jnp.bfloat16)
    summed = jax.ops.segment_sum(message.astype(jnp.float32), targets, num_segments=own_rows.shape[0]).astype(jnp.bfloat16)
    updated = (own_rows.astype(jnp.float32) + jnp.dot(summed, w_node, preferred_element_type=jnp.float32)).astype(jnp.bfloat16)
    return updated, preact


def edge_backward(grad_out, extended, own_rows, preact, sources, targets, w_send, w_recv, w_node):
    rounded = grad_out.astype(jnp.bfloat16)
    grad_sum = jnp.dot(rounded, w_node.T, preferred_element_type=jnp.float32)
    grad_pre = (grad_sum[targets] * silu_slope(preact)).astype(jnp.bfloat16)
    grad_ext = jax.ops.segment_sum(jnp.dot(grad_pre, w_send.T, preferred_element_type=jnp.float32), sources, num_segments=extended.shape[0])
    own_count = own_rows.shape[0]
    grad_own = grad_out + jax.ops.segment_sum(jnp.dot(grad_pre, w_recv.T, preferred_element_type=jnp.float32), targets, num_segments=own_count)
    grad_own = grad_own + grad_ext[:own_count]
    grad_weight = lax.dot_general(extended[sources], grad_pre, (((0,), (0,)), ((), ())), preferred_element_type=jnp.float32)
    return grad_own, grad_ext[own_count:], grad_weight


def top_forward(pooled, w_top):
    slope_in = jnp.dot(pooled.astype(jnp.bfloat16), w_top, preferred_element_type=jnp.float32)
    return (pooled + jax.nn.silu(slope_in)).astype(jnp.bfloat16), slope_in


def top_backward(grad_top, slope_in, w_top):
    inner = (grad_top * silu_slope(slope_in)).astype(jnp.bfloat16)
    return grad_top + jnp.dot(inner, w_top.T, preferred_element_type=jnp.float32)


def pick_rows(rows, index):
    return rows[index]


def add_rows(grads, index, values):
    padded = jnp.concatenate([grads, jnp.zeros((1, grads.shape[1]), jnp.float32)], axis=0)
    return padded.at[index].add(values)[:-1]


def reference(features, cotangent, fine_send, fine_rim, fine_src, fine_dst, fine_pool, coarse_send, coarse_src, coarse_dst, coarse_pool, w_send, w_recv, w_node, v_send, v_recv, v_node, w_top):
    group_count = N_GROUP
    dom_count = N_DOM
    devices = group_count * dom_count
    width = features.shape[1]
    pick = jax.vmap(jax.vmap(pick_rows))
    scatter = jax.vmap(jax.vmap(add_rows))
    feats = features.reshape(group_count, dom_count, NODE_DEV, width)
    padded = jnp.concatenate([feats, jnp.zeros((group_count, dom_count, 1, width), jnp.bfloat16)], axis=2)
    send = fine_send.reshape(group_count, dom_count, dom_count, SLOT)
    outgoing = pick(padded, send)
    incoming = jnp.swapaxes(outgoing, 1, 2).reshape(group_count, dom_count, dom_count * SLOT, width)
    layers = pick(feats, fine_rim.reshape(group_count, dom_count, 2, SLOT_G))
    blank = jnp.zeros((1, dom_count, SLOT_G, width), jnp.bfloat16)
    from_prev = jnp.concatenate([blank, layers[:-1, :, 1]], axis=0)
    from_next = jnp.concatenate([layers[1:, :, 0], blank], axis=0)
    extended = jnp.concatenate([feats, incoming, from_prev, from_next], axis=2).reshape(devices, -1, width)
    own = feats.reshape(devices, NODE_DEV, width)
    sources = fine_src.reshape(devices, EDGE_DEV)
    targets = fine_dst.reshape(devices, EDGE_DEV)

    def fine_step(item):
        return edge_forward(item[0], item[1], item[2], item[3], w_send, w_recv, w_node)[0]

    updated = lax.map(fine_step, (extended, own, sources, targets))
    coarse_total = NC_DEV * dom_count
    group_of = jnp.arange(devices * NODE_DEV, dtype=jnp.int32) // (dom_count * NODE_DEV)
    fine_ids = (group_of * coarse_total + fine_pool).astype(jnp.int32)
    pooled_fine = jax.ops.segment_sum(updated.reshape(-1, width).astype(jnp.float32), fine_ids, num_segments=group_count * coarse_total)
    coarse_in = (0.25 * pooled_fine).astype(jnp.bfloat16).reshape(group_count, dom_count, NC_DEV, width)
    cpadded = jnp.concatenate([coarse_in, jnp.zeros((group_count, dom_count, 1, width), jnp.bfloat16)], axis=2)
    csend = coarse_send.reshape(group_count, dom_count, dom_count, CSLOT)
    cincoming = jnp.swapaxes(pick(cpadded, csend), 1, 2).reshape(group_count, dom_count, dom_count * CSLOT, width)
    cextended = jnp.concatenate([coarse_in, cincoming], axis=2).reshape(devices, -1, width)
    cown = coarse_in.reshape(devices, NC_DEV, width)
    csources = coarse_src.reshape(devices, CEDGE_DEV)
    ctargets = coarse_dst.reshape(devices, CEDGE_DEV)

    def coarse_step(item):
        return edge_forward(item[0], item[1], item[2], item[3], v_send, v_recv, v_node)[0]

    coarse_mid = lax.map(coarse_step, (cextended, cown, csources, ctargets)).reshape(-1, width)
    pooled = 0.125 * jax.ops.segment_sum(coarse_mid.astype(jnp.float32), coarse_pool, num_segments=NCC)
    top_out, slope_in = top_forward(pooled, w_top)
    coarse_out = (coarse_mid.astype(jnp.float32) + top_out[coarse_pool].astype(jnp.float32)).astype(jnp.bfloat16)
    flow = (updated.reshape(-1, width).astype(jnp.float32) + coarse_out[fine_ids].astype(jnp.float32)).astype(jnp.bfloat16)

    grad_flow = cotangent.astype(jnp.float32)
    grad_coarse = jax.ops.segment_sum(grad_flow, fine_ids, num_segments=group_count * coarse_total)
    grad_top = jax.ops.segment_sum(grad_coarse, coarse_pool, num_segments=NCC)
    grad_pool = top_backward(grad_top, slope_in, w_top)
    grad_cmid = (grad_coarse + 0.125 * grad_pool[coarse_pool]).reshape(devices, NC_DEV, width)

    def coarse_back(item):
        preact = edge_forward(item[0], item[1], item[2], item[3], v_send, v_recv, v_node)[1]
        result = edge_backward(item[4], item[0], item[1], preact, item[2], item[3], v_send, v_recv, v_node)
        return result[0], result[1]

    c_own, c_halo = lax.map(coarse_back, (cextended, cown, csources, ctargets, grad_cmid))
    creturned = jnp.swapaxes(c_halo.reshape(group_count, dom_count, dom_count, CSLOT, width), 1, 2)
    creturned = creturned.reshape(group_count, dom_count, dom_count * CSLOT, width)
    grad_cin = scatter(c_own.reshape(group_count, dom_count, NC_DEV, width), csend.reshape(group_count, dom_count, dom_count * CSLOT), creturned)
    grad_fmid = (grad_flow + 0.25 * grad_cin.reshape(-1, width)[fine_ids]).reshape(devices, NODE_DEV, width)

    def fine_back(item):
        preact = edge_forward(item[0], item[1], item[2], item[3], w_send, w_recv, w_node)[1]
        return edge_backward(item[4], item[0], item[1], preact, item[2], item[3], w_send, w_recv, w_node)

    f_own, f_halo, f_weight = lax.map(fine_back, (extended, own, sources, targets, grad_fmid))
    grad_send = jnp.sum(f_weight, axis=0)
    split = dom_count * SLOT
    dom_part = f_halo[:, :split].reshape(group_count, dom_count, dom_count, SLOT, width)
    dom_back = jnp.swapaxes(dom_part, 1, 2).reshape(group_count, dom_count, dom_count * SLOT, width)
    grad_x = scatter(f_own.reshape(group_count, dom_count, NODE_DEV, width), send.reshape(group_count, dom_count, dom_count * SLOT), dom_back)
    prev_grad = f_halo[:, split:split + SLOT_G].reshape(group_count, dom_count, SLOT_G, width)
    next_grad = f_halo[:, split + SLOT_G:].reshape(group_count, dom_count, SLOT_G, width)
    blank_grad = jnp.zeros((1, dom_count, SLOT_G, width), jnp.float32)
    to_layer_one = jnp.concatenate([prev_grad[1:], blank_grad], axis=0)
    to_layer_zero = jnp.concatenate([blank_grad, next_grad[:-1]], axis=0)
    rim_values = jnp.stack([to_layer_zero, to_layer_one], axis=2).reshape(group_count, dom_count, 2 * SLOT_G, width)
    grad_x = scatter(grad_x, fine_rim.reshape(group_count, dom_count, 2 * SLOT_G), rim_values)
    return flow, grad_x.reshape(-1, width), grad_send
```

```python
import functools

import jax
import jax.numpy as jnp
from jax import lax
from jax.experimental import pallas as pl
from jax.experimental.pallas import tpu as pltpu
from jax.sharding import PartitionSpec as P

NCC = 512
BF = jnp.bfloat16
F32 = jnp.float32
NN = ((1,), (0,))
NT = ((1,), (1,))
TN = ((0,), (0,))


def dot(a, b, dims):
    return lax.dot_general(a, b, (dims, ((), ())), preferred_element_type=F32)


def hot(row, count):
    mark = lax.broadcasted_iota(jnp.int32, (count, row.shape[1]), 0) == row
    return jnp.where(mark, 1.0, 0.0).astype(BF)


def sigmoid(v):
    return 0.5 * (1.0 + jnp.tanh(0.5 * v))


def chunk_of(edges, limit):
    size = min(edges, limit)
    while edges % size:
        size //= 2
    return size


def call(kernel, outs, *args, scratch=()):
    vmem = pl.BlockSpec(memory_space=pltpu.VMEM)
    return pl.pallas_call(
        kernel,
        out_shape=[jax.ShapeDtypeStruct(shape, kind) for shape, kind in outs],
        in_specs=[vmem] * len(args),
        out_specs=[vmem] * len(outs),
        scratch_shapes=[pltpu.VMEM(shape, kind) for shape, kind in scratch],
        compiler_params=pltpu.CompilerParams(vmem_limit_bytes=56 * 1024 * 1024),
    )(*args)


def select_kernel(index_ref, rows_ref, out_ref):
    rows = rows_ref[...]
    out_ref[...] = dot(hot(index_ref[...], rows.shape[0]), rows, TN).astype(BF)


def edges_forward(src_ref, dst_ref, send_t, recv_t, slope_ref, acc_ref, size):
    rows, count = send_t.shape[1], recv_t.shape[1]
    acc_ref[...] = jnp.zeros_like(acc_ref)

    def step(i, carry):
        at = pl.ds(pl.multiple_of(i * size, size), size)
        by_dst = hot(dst_ref[:, at], count)
        pre = dot(send_t, hot(src_ref[:, at], rows), NN) + dot(recv_t, by_dst, NN)
        sigma = sigmoid(pre)
        slope_ref[:, at] = (sigma * (1.0 + pre * (1.0 - sigma))).astype(BF)
        acc_ref[...] += dot(by_dst, (pre * sigma).astype(BF), NT)
        return carry

    lax.fori_loop(0, src_ref.shape[1] // size, step, 0)


def edges_backward(src_ref, dst_ref, grad_t, slope_ref, by_src_ref, by_dst_ref, size):
    by_src_ref[...] = jnp.zeros_like(by_src_ref)
    by_dst_ref[...] = jnp.zeros_like(by_dst_ref)

    def step(i, carry):
        at = pl.ds(pl.multiple_of(i * size, size), size)
        by_dst = hot(dst_ref[:, at], by_dst_ref.shape[0])
        gpre = (dot(grad_t, by_dst, NN) * slope_ref[:, at].astype(F32)).astype(BF)
        by_src_ref[...] += dot(hot(src_ref[:, at], by_src_ref.shape[0]), gpre, NT)
        by_dst_ref[...] += dot(by_dst, gpre, NT)
        return carry

    lax.fori_loop(0, src_ref.shape[1] // size, step, 0)


def fine_forward_kernel(
    size, src_ref, dst_ref, pool_ref, ext_ref, cot_ref, send_ref, recv_ref, node_ref,
    upd_ref, part_ref, slope_ref, acc_ref,
):
    own = ext_ref[: cot_ref.shape[0], :]
    send_t = dot(send_ref[...].T, ext_ref[...], NT).astype(BF)
    recv_t = dot(recv_ref[...].T, own, NT).astype(BF)
    edges_forward(src_ref, dst_ref, send_t, recv_t, slope_ref, acc_ref, size)
    updated = (own.astype(F32) + dot(acc_ref[...].astype(BF), node_ref[...], NN)).astype(BF)
    upd_ref[...] = updated
    both = jnp.concatenate([updated, cot_ref[...]], axis=1)
    part_ref[...] = dot(hot(pool_ref[...], part_ref.shape[0]), both, NN).astype(BF)


def coarse_forward_kernel(
    size, src_ref, dst_ref, ext_ref, sums_ref, send_ref, recv_ref, node_ref,
    mid_ref, slope_ref, acc_ref,
):
    sums = sums_ref[...]
    width = acc_ref.shape[1]
    own = (0.25 * sums[:, :width].astype(F32)).astype(BF)
    send_t = dot(send_ref[...].T, own, NT).astype(BF)
    recv_t = dot(recv_ref[...].T, own, NT).astype(BF)
    send_t = dot(send_t, hot(ext_ref[...], own.shape[0]), NN).astype(BF)
    edges_forward(src_ref, dst_ref, send_t, recv_t, slope_ref, acc_ref, size)
    mid = (own.astype(F32) + dot(acc_ref[...].astype(BF), node_ref[...], NN)).astype(BF)
    mid_ref[...] = jnp.concatenate([mid, sums[:, width:]], axis=1)


def coarse_backward_kernel(
    size, src_ref, dst_ref, ext_ref, pool_ref, mids_ref, slope_ref, top_ref, send_ref, recv_ref,
    node_ref, out_ref, by_src_ref, by_dst_ref,
):
    width = by_dst_ref.shape[1]
    own_count = by_dst_ref.shape[0]
    mids = mids_ref[...]
    own = mids[:own_count].astype(F32)
    pools = hot(pool_ref[...], NCC)
    sums = dot(pools, mids, NN)
    pooled = 0.125 * sums[:, :width]
    grad_top = sums[:, width:]
    weight = top_ref[...]
    slope_in = dot(pooled.astype(BF), weight, NN)
    sigma = sigmoid(slope_in)
    top_out = (pooled + slope_in * sigma).astype(BF)
    inner = (grad_top * (sigma * (1.0 + slope_in * (1.0 - sigma)))).astype(BF)
    grad_pool = 0.125 * (grad_top + dot(inner, weight, NT))
    both = jnp.concatenate([top_out, grad_pool.astype(BF)], axis=1)
    at_node = dot(pools[:, :own_count], both, TN)
    coarse_out = (own[:, :width] + at_node[:, :width]).astype(BF)
    grad = own[:, width:] + at_node[:, width:]
    grad_t = dot(node_ref[...], grad.astype(BF), NT).astype(BF)
    edges_backward(src_ref, dst_ref, grad_t, slope_ref, by_src_ref, by_dst_ref, size)
    by_node = dot(hot(ext_ref[...], own_count), by_src_ref[...].astype(BF), NN).astype(BF)
    grad = grad + dot(by_node, send_ref[...], NT)
    grad = grad + dot(by_dst_ref[...].astype(BF), recv_ref[...], NT)
    out_ref[...] = jnp.concatenate([coarse_out, (0.25 * grad).astype(BF)], axis=1)


def fine_backward_kernel(
    size, src_ref, dst_ref, pool_ref, ext_ref, cot_ref, upd_ref, coarse_ref, slope_ref, send_ref,
    recv_ref, node_ref, flow_ref, own_ref, halo_ref, weight_ref, by_src_ref, by_dst_ref,
):
    count, width = cot_ref.shape
    at_node = dot(hot(pool_ref[...], coarse_ref.shape[0]), coarse_ref[...], TN)
    flow_ref[...] = (upd_ref[...].astype(F32) + at_node[:, :width]).astype(BF)
    grad = cot_ref[...].astype(F32) + at_node[:, width:]
    own_ref[...] = grad
    grad_t = dot(node_ref[...], grad.astype(BF), NT).astype(BF)
    edges_backward(src_ref, dst_ref, grad_t, slope_ref, by_src_ref, by_dst_ref, size)
    by_src = by_src_ref[...].astype(BF)
    grad_ext = dot(by_src, send_ref[...], NT)
    halo_ref[...] = grad_ext[count:].astype(BF)
    own_ref[...] += grad_ext[:count] + dot(by_dst_ref[...].astype(BF), recv_ref[...], NT)
    weight_ref[...] = dot(ext_ref[...], by_src, TN).astype(BF)


def return_kernel(index_ref, rows_ref, own_ref, out_ref):
    out_ref[...] = own_ref[...] + dot(hot(index_ref[...], own_ref.shape[0]), rows_ref[...], NN)


def to_xor(value, axis, offset):
    count = lax.axis_size(axis)
    return lax.ppermute(value, axis, [(i, i ^ offset) for i in range(count)])


def xor_rows(array, by):
    count = array.shape[0]
    bit = 1
    while bit < count:
        parts = array.reshape((count // (2 * bit), 2, bit) + array.shape[1:])
        array = jnp.where((by & bit) != 0, parts[:, ::-1], parts).reshape(array.shape)
        bit *= 2
    return array


def tree_sum(parts):
    parts = [part.astype(F32) for part in parts]
    while len(parts) > 1:
        parts = [a + b for a, b in zip(parts[::2], parts[1::2])]
    return parts[0]


def exchange(blocks, other, mine):
    count, rows, width = blocks.shape
    paired = jnp.moveaxis(blocks.reshape(count // 2, 2, rows, width), 1, 0)
    if other is None:
        got = to_xor(paired[1].reshape(-1, width), "dom", 1)
    else:
        got = to_xor(jnp.concatenate([paired[1].reshape(-1, width), other]), "dom", 1)
        half = (mine.astype(F32) + got[count // 2 * rows :].astype(F32)).astype(BF)
    pieces = []
    halves = [] if other is None else [half]
    for chip in range(1, count // 2):
        message = [paired[0, chip], got[chip * rows : (chip + 1) * rows]]
        if other is not None:
            message.append(half)
        landed = to_xor(jnp.concatenate(message), "dom", 2 * chip)
        pieces.append(landed[: 2 * rows])
        if other is not None:
            halves.append(landed[2 * rows :])
    arrived = jnp.concatenate([paired[0, 0], got[:rows]] + pieces)
    return arrived, (tree_sum(halves) if other is not None else None)


def local(
    features, cotangent, fine_send, fine_rim, fine_src, fine_dst, fine_pool, coarse_send,
    coarse_src, coarse_dst, coarse_pool, w_send, w_recv, w_node, v_send, v_recv, v_node, w_top,
):
    count, width = features.shape
    doms = lax.axis_size("dom")
    groups = lax.axis_size("group")
    me = lax.axis_index("dom")
    core = me & 1
    chips = doms // 2
    slots = fine_send.shape[1]
    cslots = coarse_send.shape[1]
    rim = fine_rim.shape[1]
    coarse = coarse_pool.shape[0]
    group_coarse = coarse * doms
    half_coarse = group_coarse // 2
    edges = fine_src.shape[0]
    cedges = coarse_src.shape[0]
    forward = [(i, i + 1) for i in range(groups - 1)]
    backward = [(i + 1, i) for i in range(groups - 1)]

    def place(dom):
        return (((dom & 1) ^ core) * chips + (dom >> 1)) * coarse

    table = jnp.concatenate([coarse_send.reshape(-1), coarse_src, coarse_dst, coarse_pool])
    table = lax.all_to_all(
        jnp.broadcast_to(table[None], (doms, table.shape[0])), "dom", 0, 0, tiled=True
    )
    sends = table[:, : doms * cslots].reshape(doms, doms, cslots)
    dom_ids = jnp.arange(doms, dtype=jnp.int32)
    places = place(dom_ids)
    halo_ids = jnp.where(sends < coarse, sends + places[:, None, None], -1)
    halo_ids = jnp.swapaxes(halo_ids, 0, 1).reshape(doms, doms * cslots)
    own_ids = places[:, None] + jnp.arange(coarse, dtype=jnp.int32)[None, :]
    cext_row = jnp.concatenate([own_ids, halo_ids], axis=1).reshape(1, -1)
    cext_count = coarse + doms * cslots
    at = doms * cslots
    csrc_row = (table[:, at : at + cedges] + dom_ids[:, None] * cext_count).reshape(1, -1)
    cdst_row = (table[:, at + cedges : at + 2 * cedges] + places[:, None]).reshape(1, -1)
    pools = jnp.swapaxes(table[:, at + 2 * cedges :].reshape(chips, 2, coarse), 0, 1)
    pools = jnp.where(core == 1, pools[::-1], pools).reshape(1, group_coarse)

    halo = doms * slots
    inside = (fine_src >= count) & (fine_src < count + halo)
    device, slot = (fine_src - count) // slots, (fine_src - count) % slots
    src_row = jnp.where(inside, count + (device ^ me) * slots + slot, fine_src).reshape(1, -1)
    dst_row = fine_dst.reshape(1, -1)
    pool_row = (place(fine_pool // coarse) + fine_pool % coarse).reshape(1, -1)
    out_row = jnp.concatenate(
        [xor_rows(fine_send, me).reshape(1, -1), fine_rim.reshape(1, -1)], axis=1
    )

    (rows,) = call(select_kernel, [((halo + 2 * rim, width), BF)], out_row, features)
    incoming, _ = exchange(rows[:halo].reshape(doms, slots, width), None, None)
    from_next = lax.ppermute(rows[halo : halo + rim], "group", backward)
    from_prev = lax.ppermute(rows[halo + rim :], "group", forward)
    extended = jnp.concatenate([features, incoming, from_prev, from_next], axis=0)

    size = chunk_of(edges, 1024)
    updated, part, slope = call(
        functools.partial(fine_forward_kernel, size),
        [((count, width), BF), ((group_coarse, 2 * width), BF), ((width, edges), BF)],
        src_row, dst_row, pool_row, extended, cotangent, w_send, w_recv, w_node,
        scratch=[((count, width), F32)],
    )
    got = to_xor(part[half_coarse:], "dom", 1)
    half = (part[:half_coarse].astype(F32) + got.astype(F32)).astype(BF)
    half = tree_sum([half] + [to_xor(half, "dom", 2 * o) for o in range(1, chips)]).astype(BF)
    sums = jnp.concatenate([half, to_xor(half, "dom", 1)], axis=0)

    csize = chunk_of(cedges * doms, 512)
    mid, cslope = call(
        functools.partial(coarse_forward_kernel, csize),
        [((group_coarse, 2 * width), BF), ((width, cedges * doms), BF)],
        csrc_row, cdst_row, cext_row, sums, v_send, v_recv, v_node,
        scratch=[((group_coarse, width), F32)],
    )
    lines = half_coarse // width
    ids = pools[0, :half_coarse].reshape(lines, width)
    ids = jnp.concatenate([ids >> 7, ids & 127], axis=1).astype(BF)
    ids = jnp.concatenate([ids, jnp.zeros((-lines % 16, 2 * width), BF)], axis=0)
    message = jnp.concatenate([mid[:half_coarse], ids], axis=0)
    others = [to_xor(message, "group", o) for o in range(1, groups)]
    others = jnp.stack(others)
    others = jnp.stack([others, to_xor(others, "dom", 1)])
    ids = others[:, :, half_coarse : half_coarse + lines].astype(jnp.int32)
    ids = (ids[..., :width] * 128 + ids[..., width:]).reshape(1, -1)
    mids = jnp.concatenate([mid, others[:, :, :half_coarse].reshape(-1, 2 * width)], axis=0)
    pool_all = jnp.concatenate([pools, ids], axis=1)

    (back,) = call(
        functools.partial(coarse_backward_kernel, csize),
        [((group_coarse, 2 * width), BF)],
        csrc_row, cdst_row, cext_row, pool_all, mids, cslope, w_top, v_send, v_recv, v_node,
        scratch=[((cext_row.shape[1], width), F32), ((group_coarse, width), F32)],
    )

    flow, own, halo_grad, weight = call(
        functools.partial(fine_backward_kernel, size),
        [((count, width), BF), ((count, width), F32), ((halo + 2 * rim, width), BF),
         ((width, width), BF)],
        src_row, dst_row, pool_row, extended, cotangent, updated, back, slope, w_send, w_recv,
        w_node,
        scratch=[((extended.shape[0], width), F32), ((count, width), F32)],
    )

    low, high = weight[: width // 2], weight[width // 2 :]
    mine = jnp.where(core == 1, high, low)
    other = jnp.where(core == 1, low, high)
    returned, mine = exchange(halo_grad[:halo].reshape(doms, slots, width), other, mine)
    to_first = lax.ppermute(halo_grad[halo + rim :], "group", forward)
    to_second = lax.ppermute(halo_grad[halo : halo + rim], "group", backward)
    returned = jnp.concatenate([returned, to_first, to_second], axis=0)
    (grad_x,) = call(return_kernel, [((count, width), F32)], out_row, returned, own)

    mine = mine.astype(BF)
    mine = tree_sum([mine] + [to_xor(mine, "group", o) for o in range(1, groups)])
    other = to_xor(mine, "dom", 1)
    grad_send = jnp.concatenate(
        [jnp.where(core == 1, other, mine), jnp.where(core == 1, mine, other)], axis=0
    )
    return flow, grad_x, grad_send


def solution(mesh):
    rows = P(("group", "dom"), None)
    line = P(("group", "dom"))
    placed = (rows, rows, rows, rows, line, line, line, rows, line, line, line) + (P(),) * 7
    return jax.shard_map(
        local, mesh=mesh, in_specs=placed, out_specs=(rows, rows, P()), check_vma=False
    )
```

```python
import functools

import jax
import jax.numpy as jnp
from jax import lax
from jax.experimental import pallas as pl
from jax.experimental.pallas import tpu as pltpu
from jax.sharding import PartitionSpec as P

NCC = 512
BF = jnp.bfloat16
F32 = jnp.float32
NN = ((1,), (0,))
NT = ((1,), (1,))
TN = ((0,), (0,))


def dot(a, b, dims):
    return lax.dot_general(a, b, (dims, ((), ())), preferred_element_type=F32)


def hot(row, count):
    mark = lax.broadcasted_iota(jnp.int32, (count, row.shape[1]), 0) == row
    return jnp.where(mark, 1.0, 0.0).astype(BF)


def sigmoid(v):
    return 0.5 * (1.0 + jnp.tanh(0.5 * v))


def chunk_of(edges, limit):
    size = min(edges, limit)
    while edges % size:
        size //= 2
    return size


def whole(count):
    return [pl.BlockSpec(memory_space=pltpu.VMEM)] * count


def call(kernel, outs, *args, scratch=(), extra=0):
    return pl.pallas_call(
        kernel,
        out_shape=[jax.ShapeDtypeStruct(shape, kind) for shape, kind in outs],
        in_specs=whole(len(args)),
        out_specs=whole(len(outs)),
        scratch_shapes=[pltpu.VMEM(shape, kind) for shape, kind in scratch],
        compiler_params=pltpu.CompilerParams(vmem_limit_bytes=(14 << 20) + extra),
    )(*args)


def log2(value):
    assert value & (value - 1) == 0
    return value.bit_length() - 1


def lanes(count, rows=1):
    return lax.broadcasted_iota(jnp.int32, (rows, count), 1)


def order(dom, chips):
    return (dom & 1) * chips + (dom >> 1)


def place(dom, core, chips):
    return ((dom & 1) ^ core) * chips + (dom >> 1)


def tree_sum(parts):
    parts = [part.astype(F32) for part in parts]
    while len(parts) > 1:
        parts = [a + b for a, b in zip(parts[::2], parts[1::2])]
    return parts[0]


class Payload:
    def __init__(self, cedges, group_coarse, doms):
        self.edges = cedges // 128
        self.lines = group_coarse // 128
        self.dst = self.edges
        self.high = 2 * self.edges
        self.low = self.high + self.lines
        self.send = self.low + self.lines
        self.rows = -(-(self.send + doms) // 16) * 16


def send_row(send_ref):
    doms, slots = send_ref.shape
    send = send_ref[...]
    spot = lax.broadcasted_iota(jnp.int32, (slots, doms * slots), 0)
    spread = jnp.where(lanes(doms * slots, slots) & (slots - 1) == spot, 1.0, 0.0).astype(BF)
    high = dot((send >> 4).astype(F32).astype(BF), spread, NN)
    low = dot((send & 15).astype(F32).astype(BF), spread, NN)
    value = high * 16.0 + low
    owner = lax.broadcasted_iota(jnp.int32, (doms, doms * slots), 0)
    mine = lanes(doms * slots, doms) >> log2(slots) == owner
    return jnp.sum(jnp.where(mine, value, 0.0), axis=0, keepdims=True).astype(jnp.int32)


def start_kernel(
    pay, send_ref, rim_ref, rows_ref, csrc_ref, cdst_ref, cpool_ref, csend_ref,
    odd_ref, even_ref, pay_ref, first_ref, second_ref, picked_ref, lines_ref,
):
    me = lax.axis_index("dom")
    doms, slots = send_ref.shape
    rows = rows_ref[...]
    count = rows.shape[0]
    picked_ref[...] = dot(hot(send_row(send_ref), count), rows, TN).astype(BF)
    for chip in range(doms // 2):
        here = pl.ds(chip * slots, slots)
        for part, ref in ((0, even_ref), (1, odd_ref)):
            at = pl.multiple_of(((2 * chip + part) ^ me) * slots, slots)
            ref[here, :] = picked_ref[pl.ds(at, slots), :]
    first_ref[...] = dot(hot(rim_ref[0:1, :], count), rows, TN).astype(BF)
    second_ref[...] = dot(hot(rim_ref[1:2, :], count), rows, TN).astype(BF)

    lines_ref[...] = jnp.zeros_like(lines_ref)
    lines_ref[: pay.edges, :] = csrc_ref[...].astype(F32)
    lines_ref[pay.dst : pay.dst + pay.edges, :] = cdst_ref[...].astype(F32)
    coarse = cpool_ref.shape[1]
    cslots = csend_ref.shape[1]
    pool = cpool_ref[...]
    spot = lax.broadcasted_iota(jnp.int32, (coarse, pay.lines * 128), 0)
    at = order(me, doms // 2) * coarse
    spread = jnp.where(lanes(pay.lines * 128, coarse) == spot + at, 1.0, 0.0).astype(BF)
    high = dot((pool >> 7).astype(F32).astype(BF), spread, NN)
    low = dot((pool & 127).astype(F32).astype(BF), spread, NN)
    for line in range(pay.lines):
        here = slice(line * 128, line * 128 + 128)
        lines_ref[pay.high + line : pay.high + line + 1, :] = high[:, here]
        lines_ref[pay.low + line : pay.low + line + 1, :] = low[:, here]
    spot = lax.broadcasted_iota(jnp.int32, (cslots, 128), 0)
    spread = jnp.where(lanes(128, cslots) == spot + me * cslots, 1.0, 0.0).astype(BF)
    sends = dot(csend_ref[...].astype(F32).astype(BF), spread, NN)
    lines_ref[pay.send : pay.send + doms, :] = sends
    payload = lines_ref[...].astype(BF)
    pay_ref[...] = payload
    odd_ref[doms // 2 * slots :, :] = payload


def pack_kernel(slots, even_ref, got_ref, pay_ref, *out_refs):
    chips = len(out_refs) + 1
    for chip, ref in enumerate(out_refs, 1):
        ref[:slots, :] = even_ref[chip * slots : chip * slots + slots, :]
        ref[slots : 2 * slots, :] = got_ref[chip * slots : chip * slots + slots, :]
        rows = pay_ref.shape[0]
        ref[2 * slots : 2 * slots + rows, :] = pay_ref[...]
        if ref.shape[0] > 2 * slots + rows:
            ref[2 * slots + rows :, :] = got_ref[chips * slots :, :]


def edges_forward(src_ref, dst_ref, send_t, recv_t, slope_ref, acc_ref, size):
    rows, count = send_t.shape[1], recv_t.shape[1]
    acc_ref[...] = jnp.zeros_like(acc_ref)

    def step(i, carry):
        at = pl.ds(pl.multiple_of(i * size, size), size)
        by_dst = hot(dst_ref[:, at], count)
        pre = dot(send_t, hot(src_ref[:, at], rows), NN) + dot(recv_t, by_dst, NN)
        sigma = sigmoid(pre)
        slope_ref[:, at] = (sigma * (1.0 + pre * (1.0 - sigma))).astype(BF)
        acc_ref[...] += dot(by_dst, (pre * sigma).astype(BF), NT)
        return carry

    lax.fori_loop(0, src_ref.shape[1] // size, step, 0)


def edges_backward(src_ref, dst_ref, grad_t, slope_ref, by_src_ref, by_dst_ref, size):
    by_src_ref[...] = jnp.zeros_like(by_src_ref)
    by_dst_ref[...] = jnp.zeros_like(by_dst_ref)

    def step(i, carry):
        at = pl.ds(pl.multiple_of(i * size, size), size)
        by_dst = hot(dst_ref[:, at], by_dst_ref.shape[0])
        gpre = (dot(grad_t, by_dst, NN) * slope_ref[:, at].astype(F32)).astype(BF)
        by_src_ref[...] += dot(hot(src_ref[:, at], by_src_ref.shape[0]), gpre, NT)
        by_dst_ref[...] += dot(by_dst, gpre, NT)
        return carry

    lax.fori_loop(0, src_ref.shape[1] // size, step, 0)


def fine_forward_kernel(
    size, slots, coarse, src_ref, dst_ref, pool_ref, rows_ref, even_ref, got_ref, prev_ref,
    next_ref, cot_ref, send_ref, recv_ref, node_ref, *refs,
):
    chips = even_ref.shape[0] // slots
    landed = refs[: chips - 1]
    (upd_ref, mine_ref, other_ref, slope_ref, ext_ref, src_row_ref, pool_row_ref,
     acc_ref) = refs[chips - 1 :]
    me = lax.axis_index("dom")
    count, width = cot_ref.shape
    halo = 2 * chips * slots
    rim = prev_ref.shape[0]
    ext_ref[:count, :] = rows_ref[...]
    ext_ref[count : count + slots, :] = even_ref[:slots, :]
    ext_ref[count + slots : count + 2 * slots, :] = got_ref[:slots, :]
    for chip, ref in enumerate(landed, 1):
        at = count + 2 * chip * slots
        ext_ref[at : at + 2 * slots, :] = ref[: 2 * slots, :]
    ext_ref[count + halo : count + halo + rim, :] = prev_ref[...]
    ext_ref[count + halo + rim :, :] = next_ref[...]

    log2(slots)
    src = src_ref[...]
    inside = (src >= count) & (src < count + halo)
    src_row_ref[...] = jnp.where(inside, count + ((src - count) ^ (me * slots)), src)
    pool = pool_ref[...]
    bits = log2(coarse)
    pool_row = place(pool >> bits, me & 1, chips) * coarse + (pool & (coarse - 1))
    pool_row_ref[...] = pool_row

    own = rows_ref[...]
    send_t = dot(send_ref[...].T, ext_ref[...], NT).astype(BF)
    recv_t = dot(recv_ref[...].T, own, NT).astype(BF)
    edges_forward(src_row_ref, dst_ref, send_t, recv_t, slope_ref, acc_ref, size)
    updated = (own.astype(F32) + dot(acc_ref[...].astype(BF), node_ref[...], NN)).astype(BF)
    upd_ref[...] = updated
    both = jnp.concatenate([updated, cot_ref[...]], axis=1)
    half = mine_ref.shape[0]
    part = dot(hot(pool_row, 2 * half), both, NN).astype(BF)
    mine_ref[...] = part[:half]
    other_ref[...] = part[half:]


def add_kernel(out_ref_first, *refs):
    *parts, out_ref = (out_ref_first,) + refs
    out_ref[...] = tree_sum([part[...] for part in parts]).astype(out_ref.dtype)


def coarse_forward_kernel(
    pay, size, coarse, mine_ref, other_ref, send_ref, recv_ref, node_ref, pay_ref, got_ref, *refs
):
    (*landed, message_ref, mid_ref, slope_ref, src_ref, dst_ref, ext_ref, pool_ref, acc_ref,
     sends_ref, highs_ref, lows_ref) = refs
    me = lax.axis_index("dom")
    core = me & 1
    rows = pay.rows
    chips = len(landed) + 1
    doms = 2 * chips
    half, both_width = mine_ref.shape
    width = both_width // 2
    group_coarse = 2 * half
    skip = got_ref.shape[0] - rows
    slots2 = landed[0].shape[0] - 2 * rows
    payloads = [pay_ref[...], got_ref[skip:, :]]
    for ref in landed:
        payloads += [ref[slots2 : slots2 + rows, :], ref[slots2 + rows :, :]]
    payloads = [payload.astype(F32) for payload in payloads]

    cedges = pay.edges * 128
    cslots_all = ext_ref.shape[1] // doms
    for j, payload in enumerate(payloads):
        spot = place(me ^ j, core, chips) * coarse
        for line in range(pay.edges):
            here = slice(j * cedges + line * 128, j * cedges + line * 128 + 128)
            src = payload[line : line + 1, :].astype(jnp.int32)
            away = group_coarse + j * cslots_all - coarse
            src_ref[:, here] = src + jnp.where(src < coarse, spot, away)
            dst = payload[pay.dst + line : pay.dst + line + 1, :].astype(jnp.int32)
            dst_ref[:, here] = dst + spot
    total = tree_sum(payloads)
    sends_ref[...] = total[pay.send : pay.send + doms, :]
    owner = lanes(128) >> log2(cslots_all // doms)
    spots = place(owner, core, chips) * coarse
    per_line = 128 // cslots_all
    for line in range(doms // per_line):
        joined = jnp.full((1, 128), -1, jnp.int32)
        for part in range(per_line):
            dom = me ^ (line * per_line + part)
            row = sends_ref[pl.ds(dom, 1), :].astype(jnp.int32)
            row = jnp.where(row < coarse, row + spots, -1)
            if part:
                row = pltpu.roll(row, part * cslots_all, 1)
            joined = jnp.where(lanes(128) // cslots_all == part, row, joined)
        ext_ref[:, line * 128 : line * 128 + 128] = joined
    highs_ref[...] = total[pay.high : pay.high + pay.lines, :]
    lows_ref[...] = total[pay.low : pay.low + pay.lines, :]
    upper = pay.lines // 2
    message_ref[half:, :] = jnp.zeros_like(message_ref[half:, :])
    high_rows, low_rows = [], []
    for line in range(pay.lines):
        at = pl.ds((line + core * upper) & (pay.lines - 1), 1)
        high, low = highs_ref[at, :], lows_ref[at, :]
        pool_ref[:, line * 128 : line * 128 + 128] = (high * 128.0 + low).astype(jnp.int32)
        if line < upper:
            high_rows.append(high)
            low_rows.append(low)
    tail = message_ref.shape[0] - half - upper
    zeros = [jnp.zeros((tail, 128), F32)]
    ids = jnp.concatenate(
        [jnp.concatenate(high_rows + zeros, axis=0), jnp.concatenate(low_rows + zeros, axis=0)],
        axis=1,
    )
    message_ref[half:, :] = ids.astype(BF)

    mid_ref[:half, :] = mine_ref[...]
    mid_ref[half:, :] = other_ref[...]
    own = (0.25 * mid_ref[:, :width].astype(F32)).astype(BF)
    send_t = dot(send_ref[...].T, own, NT).astype(BF)
    recv_t = dot(recv_ref[...].T, own, NT).astype(BF)
    away = dot(send_t, hot(ext_ref[...], group_coarse), NN).astype(BF)
    send_t = jnp.concatenate([send_t, away], axis=1)
    edges_forward(src_ref, dst_ref, send_t, recv_t, slope_ref, acc_ref, size)
    mid = (own.astype(F32) + dot(acc_ref[...].astype(BF), node_ref[...], NN)).astype(BF)
    mid_ref[:, :width] = mid
    message_ref[:half, :width] = mid[:half]
    message_ref[:half, width:] = mine_ref[:, width:]


def coarse_backward_kernel(
    size, src_ref, dst_ref, ext_ref, pool_ref, mid_ref, slope_ref, top_ref, send_ref, recv_ref,
    node_ref, *refs,
):
    *others, out_ref, by_src_ref, by_dst_ref, mids_ref = refs
    own_count, width = by_dst_ref.shape
    half = own_count // 2
    mids_ref[:own_count, :] = mid_ref[...]
    rows = [pool_ref[...]]
    for i, ref in enumerate(others):
        mids_ref[own_count + i * half : own_count + i * half + half, :] = ref[:half, :]
        ids = ref[half:, :].astype(F32)
        for line in range(half // 128):
            high, low = ids[line : line + 1, :128], ids[line : line + 1, 128:]
            rows.append((high * 128.0 + low).astype(jnp.int32))
    mids = mids_ref[...]
    own = mid_ref[...].astype(F32)
    pools = hot(jnp.concatenate(rows, axis=1), NCC)
    sums = dot(pools, mids, NN)
    pooled = 0.125 * sums[:, :width]
    grad_top = sums[:, width:]
    weight = top_ref[...]
    slope_in = dot(pooled.astype(BF), weight, NN)
    sigma = sigmoid(slope_in)
    top_out = (pooled + slope_in * sigma).astype(BF)
    inner = (grad_top * (sigma * (1.0 + slope_in * (1.0 - sigma)))).astype(BF)
    grad_pool = 0.125 * (grad_top + dot(inner, weight, NT))
    both = jnp.concatenate([top_out, grad_pool.astype(BF)], axis=1)
    at_node = dot(pools[:, :own_count], both, TN)
    coarse_out = (own[:, :width] + at_node[:, :width]).astype(BF)
    grad = own[:, width:] + at_node[:, width:]
    grad_t = dot(node_ref[...], grad.astype(BF), NT).astype(BF)
    edges_backward(src_ref, dst_ref, grad_t, slope_ref, by_src_ref, by_dst_ref, size)
    by_src = by_src_ref[...]
    away = dot(hot(ext_ref[...], own_count), by_src[own_count:].astype(BF), NN)
    grad = grad + dot((by_src[:own_count] + away).astype(BF), send_ref[...], NT)
    grad = grad + dot(by_dst_ref[...].astype(BF), recv_ref[...], NT)
    out_ref[...] = jnp.concatenate([coarse_out, (0.25 * grad).astype(BF)], axis=1)


def fine_backward_kernel(
    size, slots, src_ref, dst_ref, pool_ref, ext_ref, cot_ref, upd_ref, coarse_ref, slope_ref,
    send_ref, recv_ref, node_ref, flow_ref, own_ref, odd_ref, even_ref, weight_ref, prev_ref,
    next_ref, by_src_ref, by_dst_ref, all_ref,
):
    core = lax.axis_index("dom") & 1
    count, width = cot_ref.shape
    at_node = dot(hot(pool_ref[...], coarse_ref.shape[0]), coarse_ref[...], TN)
    flow_ref[...] = (upd_ref[...].astype(F32) + at_node[:, :width]).astype(BF)
    grad = cot_ref[...].astype(F32) + at_node[:, width:]
    own_ref[...] = grad
    grad_t = dot(node_ref[...], grad.astype(BF), NT).astype(BF)
    edges_backward(src_ref, dst_ref, grad_t, slope_ref, by_src_ref, by_dst_ref, size)
    by_src = by_src_ref[...].astype(BF)
    grad_ext = dot(by_src, send_ref[...], NT)
    away = grad_ext[count:].astype(BF)
    pairs = even_ref.shape[0] // slots
    for chip in range(pairs):
        at = 2 * chip * slots
        even_ref[chip * slots : chip * slots + slots, :] = away[at : at + slots]
        odd_ref[chip * slots : chip * slots + slots, :] = away[at + slots : at + 2 * slots]
    halo = 2 * pairs * slots
    rim = prev_ref.shape[0]
    prev_ref[...] = away[halo : halo + rim]
    next_ref[...] = away[halo + rim :]
    own_ref[...] += grad_ext[:count] + dot(by_dst_ref[...].astype(BF), recv_ref[...], NT)
    all_ref[...] = dot(ext_ref[...], by_src, TN)
    half = width // 2
    weight_ref[...] = all_ref[pl.ds(pl.multiple_of(core * half, half), half), :].astype(BF)
    there = pl.ds(pl.multiple_of((1 - core) * half, half), half)
    odd_ref[pairs * slots :, :] = all_ref[there, :].astype(BF)


def pack_back_kernel(slots, even_ref, got_ref, weight_ref, *refs):
    *out_refs, half_ref = refs
    chips = len(out_refs) + 1
    half = weight_ref[...].astype(F32) + got_ref[chips * slots :, :].astype(F32)
    half_ref[...] = half.astype(BF)
    for chip, ref in enumerate(out_refs, 1):
        ref[:slots, :] = even_ref[chip * slots : chip * slots + slots, :]
        ref[slots : 2 * slots, :] = got_ref[chip * slots : chip * slots + slots, :]
        ref[2 * slots :, :] = half.astype(BF)


def weight_kernel(skip, half_ref, *refs):
    *landed, out_ref = refs
    parts = [half_ref[...]] + [ref[skip:, :] for ref in landed]
    out_ref[...] = tree_sum(parts).astype(BF)


def return_kernel(
    send_ref, rim_ref, own_ref, even_ref, got_ref, first_ref, second_ref, *refs
):
    *landed, out_ref, rows_ref = refs
    me = lax.axis_index("dom")
    doms, slots = send_ref.shape
    pieces = [even_ref[:slots, :], got_ref[:slots, :]]
    for ref in landed:
        pieces += [ref[:slots, :], ref[slots : 2 * slots, :]]
    for j, piece in enumerate(pieces):
        rows_ref[pl.ds(pl.multiple_of((me ^ j) * slots, slots), slots), :] = piece
    count = own_ref.shape[0]
    total = own_ref[...] + dot(hot(send_row(send_ref), count), rows_ref[...], NN)
    total = total + dot(hot(rim_ref[0:1, :], count), first_ref[...], NN)
    out_ref[...] = total + dot(hot(rim_ref[1:2, :], count), second_ref[...], NN)


def join_kernel(mine_ref, other_ref, out_ref):
    core = lax.axis_index("dom") & 1
    half = mine_ref.shape[0]
    out_ref[pl.ds(pl.multiple_of(core * half, half), half), :] = mine_ref[...]
    out_ref[pl.ds(pl.multiple_of((1 - core) * half, half), half), :] = other_ref[...]


def to_xor(value, axis, offset):
    count = lax.axis_size(axis)
    return lax.ppermute(value, axis, [(i, i ^ offset) for i in range(count)])


def local(
    features, cotangent, fine_send, fine_rim, fine_src, fine_dst, fine_pool, coarse_send,
    coarse_src, coarse_dst, coarse_pool, w_send, w_recv, w_node, v_send, v_recv, v_node, w_top,
):
    count, width = features.shape
    doms = lax.axis_size("dom")
    groups = lax.axis_size("group")
    chips = doms // 2
    slots = fine_send.shape[1]
    cslots = coarse_send.shape[1]
    rim = fine_rim.shape[1]
    coarse = coarse_pool.shape[0]
    group_coarse = coarse * doms
    half_coarse = group_coarse // 2
    edges = fine_src.shape[0]
    cedges = coarse_src.shape[0]
    forward = [(i, i + 1) for i in range(groups - 1)]
    backward = [(i + 1, i) for i in range(groups - 1)]
    ext_count = count + doms * slots + 2 * rim
    cext_count = group_coarse + doms * doms * cslots
    pay = Payload(cedges, group_coarse, doms)
    assert coarse + doms * cslots <= 256 and doms * cslots <= 128 and width == 128
    src_row = fine_src.reshape(1, -1)
    dst_row = fine_dst.reshape(1, -1)

    odd, even, payload, first, second = call(
        functools.partial(start_kernel, pay),
        [((chips * slots + pay.rows, width), BF), ((chips * slots, width), BF),
         ((pay.rows, width), BF), ((rim, width), BF), ((rim, width), BF)],
        fine_send, fine_rim, features, coarse_src.reshape(-1, 128), coarse_dst.reshape(-1, 128),
        coarse_pool.reshape(1, -1), coarse_send,
        scratch=[((doms * slots, width), BF), ((pay.rows, 128), F32)],
    )
    got = to_xor(odd, "dom", 1)
    messages = call(
        functools.partial(pack_kernel, slots),
        [((2 * slots + 2 * pay.rows, width), BF)] * (chips - 1), even, got, payload,
    )
    landed = [to_xor(message, "dom", 2 * o) for o, message in enumerate(messages, 1)]
    from_next = lax.ppermute(first, "group", backward)
    from_prev = lax.ppermute(second, "group", forward)

    size = chunk_of(edges, 1024)
    updated, mine, other, slope, extended, src_row, pool_row = call(
        functools.partial(fine_forward_kernel, size, slots, coarse),
        [((count, width), BF), ((half_coarse, 2 * width), BF), ((half_coarse, 2 * width), BF),
         ((width, edges), BF), ((ext_count, width), BF), ((1, edges), jnp.int32),
         ((1, count), jnp.int32)],
        src_row, dst_row, fine_pool.reshape(1, -1), features, even, got, from_prev, from_next,
        cotangent, w_send, w_recv, w_node, *landed,
        scratch=[((count, width), F32)],
    )
    half_sum = [((half_coarse, 2 * width), BF)]
    (mine,) = call(add_kernel, half_sum, mine, to_xor(other, "dom", 1))
    parts = [to_xor(mine, "dom", 2 * o) for o in range(1, chips)]
    (mine,) = call(add_kernel, half_sum, mine, *parts)
    other = to_xor(mine, "dom", 1)

    csize = chunk_of(cedges * doms, 512)
    extra = 3 * cext_count * 2 * max(csize, group_coarse)
    tail = -(-(pay.lines // 2) // 16) * 16
    message, mid, cslope, csrc_row, cdst_row, cext_row, pools = call(
        functools.partial(coarse_forward_kernel, pay, csize, coarse),
        [((half_coarse + tail, 2 * width), BF), ((group_coarse, 2 * width), BF),
         ((width, cedges * doms), BF), ((1, cedges * doms), jnp.int32),
         ((1, cedges * doms), jnp.int32), ((1, doms * doms * cslots), jnp.int32),
         ((1, group_coarse), jnp.int32)],
        mine, other, v_send, v_recv, v_node, payload, got, *landed,
        scratch=[((group_coarse, width), F32), ((doms, 128), F32), ((pay.lines, 128), F32),
                 ((pay.lines, 128), F32)],
        extra=extra,
    )
    others = [to_xor(message, "group", o) for o in range(1, groups)]
    others += [to_xor(part, "dom", 1) for part in others]
    (back,) = call(
        functools.partial(coarse_backward_kernel, csize),
        [((group_coarse, 2 * width), BF)],
        csrc_row, cdst_row, cext_row, pools, mid, cslope, w_top, v_send, v_recv, v_node, *others,
        scratch=[((cext_count, width), F32), ((group_coarse, width), F32),
                 ((groups * group_coarse, 2 * width), BF)],
        extra=extra,
    )

    half = width // 2
    flow, own, odd, even, weight, prev_grad, next_grad = call(
        functools.partial(fine_backward_kernel, size, slots),
        [((count, width), BF), ((count, width), F32), ((chips * slots + half, width), BF),
         ((chips * slots, width), BF), ((half, width), BF), ((rim, width), BF),
         ((rim, width), BF)],
        src_row, dst_row, pool_row, extended, cotangent, updated, back, slope, w_send, w_recv,
        w_node,
        scratch=[((ext_count, width), F32), ((count, width), F32), ((width, width), F32)],
    )

    got = to_xor(odd, "dom", 1)
    *messages, weight = call(
        functools.partial(pack_back_kernel, slots),
        [((2 * slots + half, width), BF)] * (chips - 1) + [((half, width), BF)],
        even, got, weight,
    )
    landed = [to_xor(message, "dom", 2 * o) for o, message in enumerate(messages, 1)]
    to_first = lax.ppermute(next_grad, "group", forward)
    to_second = lax.ppermute(prev_grad, "group", backward)
    (weight,) = call(
        functools.partial(weight_kernel, 2 * slots), [((half, width), BF)], weight, *landed
    )
    parts = [to_xor(weight, "group", o) for o in range(1, groups)]
    (grad_x,) = call(
        return_kernel, [((count, width), F32)],
        fine_send, fine_rim, own, even, got, to_first, to_second, *landed,
        scratch=[((doms * slots, width), BF)],
    )
    (weight,) = call(add_kernel, [((half, width), F32)], weight, *parts)
    (grad_send,) = call(
        join_kernel, [((width, width), F32)], weight, to_xor(weight, "dom", 1)
    )
    return flow, grad_x, grad_send


def solution(mesh):
    rows = P(("group", "dom"), None)
    line = P(("group", "dom"))
    placed = (rows, rows, rows, rows, line, line, line, rows, line, line, line) + (P(),) * 7
    return jax.shard_map(
        local, mesh=mesh, in_specs=placed, out_specs=(rows, rows, P()), check_vma=False
    )
```

```python
import functools

import jax
import jax.numpy as jnp
from jax import lax
from jax.experimental import pallas as pl
from jax.experimental.pallas import tpu as pltpu
from jax.sharding import PartitionSpec as P

NCC = 512
LONG = 20_000_000_000
BF = jnp.bfloat16
F32 = jnp.float32
NN = ((1,), (0,))
NT = ((1,), (1,))
TN = ((0,), (0,))


def dot(a, b, dims):
    return lax.dot_general(a, b, (dims, ((), ())), preferred_element_type=F32)


def hot(row, count):
    mark = lax.broadcasted_iota(jnp.int32, (count, row.shape[1]), 0) == row
    return jnp.where(mark, 1.0, 0.0).astype(BF)


def sigmoid(v):
    return 0.5 * (1.0 + jnp.tanh(0.5 * v))


def chunk_of(edges, limit):
    size = 1 << (min(edges, limit).bit_length() - 1)
    while edges % size:
        size //= 2
    return size


def whole(count):
    return [pl.BlockSpec(memory_space=pltpu.VMEM)] * count


def call(kernel, outs, *args, scratch=(), extra=0, cost=0):
    return pl.pallas_call(
        kernel,
        out_shape=[jax.ShapeDtypeStruct(shape, kind) for shape, kind in outs],
        in_specs=whole(len(args)),
        out_specs=whole(len(outs)),
        scratch_shapes=[pltpu.VMEM(shape, kind) for shape, kind in scratch],
        compiler_params=pltpu.CompilerParams(vmem_limit_bytes=(14 << 20) + extra),
        cost_estimate=pl.CostEstimate(flops=cost, bytes_accessed=0, transcendentals=0),
    )(*args)


def log2(value):
    assert value & (value - 1) == 0
    return value.bit_length() - 1


def lanes(count, rows=1):
    return lax.broadcasted_iota(jnp.int32, (rows, count), 1)


def order(dom, chips):
    return (dom & 1) * chips + (dom >> 1)


def place(dom, core, chips):
    return ((dom & 1) ^ core) * chips + (dom >> 1)


def tree_sum(parts):
    parts = [part.astype(F32) for part in parts]
    while len(parts) > 1:
        parts = [a + b for a, b in zip(parts[::2], parts[1::2])]
    return parts[0]


class Payload:
    def __init__(self, cedges, group_coarse, doms):
        self.edges = cedges // 128
        self.lines = group_coarse // 128
        self.dst = self.edges
        self.high = 2 * self.edges
        self.low = self.high + self.lines
        self.send = self.low + self.lines
        self.rows = -(-(self.send + doms) // 16) * 16


def send_row(send_ref):
    doms, slots = send_ref.shape
    send = send_ref[...]
    spot = lax.broadcasted_iota(jnp.int32, (slots, doms * slots), 0)
    spread = jnp.where(lanes(doms * slots, slots) & (slots - 1) == spot, 1.0, 0.0).astype(BF)
    high = dot((send >> 4).astype(F32).astype(BF), spread, NN)
    low = dot((send & 15).astype(F32).astype(BF), spread, NN)
    value = high * 16.0 + low
    owner = lax.broadcasted_iota(jnp.int32, (doms, doms * slots), 0)
    mine = lanes(doms * slots, doms) >> log2(slots) == owner
    return jnp.sum(jnp.where(mine, value, 0.0), axis=0, keepdims=True).astype(jnp.int32)


def where_kernel(out_ref):
    out_ref[...] = jnp.full(out_ref.shape, lax.axis_index("dom"), jnp.int32)


def start_kernel(
    pay, me_ref, send_ref, rim_ref, csrc_ref, cdst_ref, cpool_ref, csend_ref, pool_ref, rows_ref,
    odd_ref, even_ref, pay_ref, near_ref, far_ref, pool_row_ref, picked_ref, lines_ref,
):
    me = lax.axis_index("dom")
    odd_group = lax.axis_index("group") & 1
    doms, slots = send_ref.shape
    rows = rows_ref[...]
    count = rows.shape[0]
    picked_ref[...] = dot(hot(send_row(send_ref), count), rows, TN).astype(BF)
    for chip in range(doms // 2):
        here = pl.ds(chip * slots, slots)
        for part, ref in ((0, even_ref), (1, odd_ref)):
            at = pl.multiple_of(((2 * chip + part) ^ me) * slots, slots)
            ref[here, :] = picked_ref[pl.ds(at, slots), :]
    near_ref[...] = dot(hot(rim_ref[pl.ds(1 - odd_group, 1), :], count), rows, TN).astype(BF)
    far_ref[...] = dot(hot(rim_ref[pl.ds(odd_group, 1), :], count), rows, TN).astype(BF)

    lines_ref[...] = jnp.zeros_like(lines_ref)
    lines_ref[: pay.edges, :] = csrc_ref[...].astype(F32)
    lines_ref[pay.dst : pay.dst + pay.edges, :] = cdst_ref[...].astype(F32)
    coarse = cpool_ref.shape[1]
    cslots = csend_ref.shape[0]
    pool = pool_ref[...]
    at = place(pool >> log2(coarse), me_ref[0:1, 0:1] & 1, doms // 2) * coarse
    pool_row_ref[...] = at + (pool & (coarse - 1))
    pool = cpool_ref[...]
    spot = lax.broadcasted_iota(jnp.int32, (coarse, pay.lines * 128), 0)
    at = order(me, doms // 2) * coarse
    spread = jnp.where(lanes(pay.lines * 128, coarse) == spot + at, 1.0, 0.0).astype(BF)
    high = dot((pool >> 7).astype(F32).astype(BF), spread, NN)
    low = dot((pool & 127).astype(F32).astype(BF), spread, NN)
    for line in range(pay.lines):
        here = slice(line * 128, line * 128 + 128)
        lines_ref[pay.high + line : pay.high + line + 1, :] = high[:, here]
        lines_ref[pay.low + line : pay.low + line + 1, :] = low[:, here]
    spot = lax.broadcasted_iota(jnp.int32, (cslots, 128), 0)
    spread = jnp.where(lanes(128, cslots) == spot + me * cslots, 1.0, 0.0).astype(BF)
    sends = dot(csend_ref[...].astype(F32).astype(BF), spread, TN)
    lines_ref[pay.send : pay.send + doms, :] = sends
    payload = lines_ref[...].astype(BF)
    pay_ref[...] = payload
    odd_ref[doms // 2 * slots :, :] = payload


def pack_kernel(slots, even_ref, got_ref, pay_ref, *out_refs):
    chips = len(out_refs) + 1
    for chip, ref in enumerate(out_refs, 1):
        ref[:slots, :] = even_ref[chip * slots : chip * slots + slots, :]
        ref[slots : 2 * slots, :] = got_ref[chip * slots : chip * slots + slots, :]
        rows = pay_ref.shape[0]
        ref[2 * slots : 2 * slots + rows, :] = pay_ref[...]
        if ref.shape[0] > 2 * slots + rows:
            ref[2 * slots + rows :, :] = got_ref[chips * slots :, :]


def edges_forward(src_ref, dst_ref, send_t, recv_t, slope_ref, acc_ref, size, known=None):
    rows, count = send_t.shape[1], acc_ref.shape[0]
    acc_ref[...] = jnp.zeros_like(acc_ref)

    def step(i, carry):
        at = pl.ds(pl.multiple_of(i * size, size), size)
        by_dst = hot(dst_ref[:, at], count)
        pre = dot(send_t, hot(src_ref[:, at], rows), NN)
        pre = pre + (dot(recv_t, by_dst, NN) if known is None else known[:, at])
        sigma = sigmoid(pre)
        slope_ref[:, at] = (sigma * (1.0 + pre * (1.0 - sigma))).astype(BF)
        acc_ref[...] += dot(by_dst, (pre * sigma).astype(BF), NT)
        return carry

    lax.fori_loop(0, src_ref.shape[1] // size, step, 0)


def edges_backward(
    src_ref, dst_ref, grad_t, slope_ref, by_src_ref, by_dst_ref, size, gpre_ref=None
):
    by_src_ref[...] = jnp.zeros_like(by_src_ref)
    if gpre_ref is None:
        by_dst_ref[...] = jnp.zeros_like(by_dst_ref)

    def step(i, carry):
        at = pl.ds(pl.multiple_of(i * size, size), size)
        by_dst = hot(dst_ref[:, at], grad_t.shape[1])
        gpre = (dot(grad_t, by_dst, NN) * slope_ref[:, at].astype(F32)).astype(BF)
        by_src_ref[...] += dot(hot(src_ref[:, at], by_src_ref.shape[0]), gpre, NT)
        if gpre_ref is None:
            by_dst_ref[...] += dot(by_dst, gpre, NT)
        else:
            gpre_ref[:, at] = gpre
        return carry

    lax.fori_loop(0, src_ref.shape[1] // size, step, 0)


def fine_local_kernel(size, src_ref, dst_ref, rows_ref, send_ref, recv_ref, known_ref):
    rows = rows_ref[...]
    count = rows.shape[0]
    send_t = dot(send_ref[...].T, rows, NT).astype(BF)
    recv_t = dot(recv_ref[...].T, rows, NT).astype(BF)

    def step(i, carry):
        at = pl.ds(pl.multiple_of(i * size, size), size)
        known = dot(send_t, hot(src_ref[:, at], count), NN)
        known_ref[:, at] = known + dot(recv_t, hot(dst_ref[:, at], count), NN)
        return carry

    lax.fori_loop(0, src_ref.shape[1] // size, step, 0)


def fine_forward_kernel(
    size, slots, src_ref, dst_ref, pool_ref, rows_ref, even_ref, got_ref, near_ref,
    far_ref, cot_ref, send_ref, known_ref, node_ref, *refs,
):
    chips = even_ref.shape[0] // slots
    landed = refs[: chips - 1]
    (upd_ref, mine_ref, other_ref, slope_ref, ext_ref, src_row_ref, acc_ref,
     away_ref) = refs[chips - 1 :]
    me = lax.axis_index("dom")
    count, _ = cot_ref.shape
    halo = 2 * chips * slots
    rim = near_ref.shape[0]
    ext_ref[:count, :] = rows_ref[...]
    ext_ref[count : count + slots, :] = even_ref[:slots, :]
    ext_ref[count + slots : count + 2 * slots, :] = got_ref[:slots, :]
    for chip, ref in enumerate(landed, 1):
        at = count + 2 * chip * slots
        ext_ref[at : at + 2 * slots, :] = ref[: 2 * slots, :]
    odd_group = lax.axis_index("group") & 1
    near, far = rim_spots(count + halo, rim, odd_group)
    ext_ref[near, :] = near_ref[...]
    ext_ref[far, :] = far_ref[...]

    src = src_ref[...]
    inside = (src >= count) & (src < count + halo)
    src = jnp.where(inside, count + ((src - count) ^ (me * slots)), src)
    src_row_ref[...] = src
    away_ref[...] = src - count

    own = rows_ref[...]
    send_t = dot(send_ref[...].T, ext_ref[count:, :], NT).astype(BF)
    edges_forward(away_ref, dst_ref, send_t, None, slope_ref, acc_ref, size, known_ref)
    updated = (own.astype(F32) + dot(acc_ref[...].astype(BF), node_ref[...], NN)).astype(BF)
    upd_ref[...] = updated
    both = jnp.concatenate([updated, cot_ref[...]], axis=1)
    half = mine_ref.shape[0]
    part = dot(hot(pool_ref[...], 2 * half), both, NN).astype(BF)
    mine_ref[...] = part[:half]
    other_ref[...] = part[half:]


def rim_spots(at, rim, odd_group):
    near = pl.multiple_of(at + (1 - odd_group) * rim, 16)
    far = pl.multiple_of(at + odd_group * rim, 16)
    return pl.ds(near, rim), pl.ds(far, rim)


def add_kernel(out_ref_first, *refs):
    *parts, out_ref = (out_ref_first,) + refs
    out_ref[...] = tree_sum([part[...] for part in parts]).astype(out_ref.dtype)


def coarse_forward_kernel(
    pay, size, coarse, mine_ref, other_ref, send_ref, recv_ref, node_ref, pay_ref, got_ref, *refs
):
    (*landed, message_ref, mid_ref, slope_ref, src_ref, dst_ref, ext_ref, pool_ref, acc_ref,
     sends_ref, highs_ref, lows_ref) = refs
    me = lax.axis_index("dom")
    core = me & 1
    rows = pay.rows
    chips = len(landed) + 1
    doms = 2 * chips
    half, both_width = mine_ref.shape
    width = both_width // 2
    group_coarse = 2 * half
    skip = got_ref.shape[0] - rows
    slots2 = landed[0].shape[0] - 2 * rows
    payloads = [pay_ref[...], got_ref[skip:, :]]
    for ref in landed:
        payloads += [ref[slots2 : slots2 + rows, :], ref[slots2 + rows :, :]]
    payloads = [payload.astype(F32) for payload in payloads]

    cedges = pay.edges * 128
    cslots_all = ext_ref.shape[1] // doms
    for j, payload in enumerate(payloads):
        spot = place(me ^ j, core, chips) * coarse
        for line in range(pay.edges):
            here = slice(j * cedges + line * 128, j * cedges + line * 128 + 128)
            src = payload[line : line + 1, :].astype(jnp.int32)
            away = group_coarse + j * cslots_all - coarse
            src_ref[:, here] = src + jnp.where(src < coarse, spot, away)
            dst = payload[pay.dst + line : pay.dst + line + 1, :].astype(jnp.int32)
            dst_ref[:, here] = dst + spot
    total = tree_sum(payloads)
    sends_ref[...] = total[pay.send : pay.send + doms, :]
    owner = lanes(128) >> log2(cslots_all // doms)
    spots = place(owner, core, chips) * coarse
    per_line = 128 // cslots_all
    for line in range(doms // per_line):
        joined = jnp.full((1, 128), -1, jnp.int32)
        for part in range(per_line):
            dom = me ^ (line * per_line + part)
            row = sends_ref[pl.ds(dom, 1), :].astype(jnp.int32)
            row = jnp.where(row < coarse, row + spots, -1)
            if part:
                row = pltpu.roll(row, part * cslots_all, 1)
            joined = jnp.where(lanes(128) // cslots_all == part, row, joined)
        ext_ref[:, line * 128 : line * 128 + 128] = joined
    highs_ref[...] = total[pay.high : pay.high + pay.lines, :]
    lows_ref[...] = total[pay.low : pay.low + pay.lines, :]
    upper = pay.lines // 2
    message_ref[half:, :] = jnp.zeros_like(message_ref[half:, :])
    high_rows, low_rows = [], []
    for line in range(pay.lines):
        at = pl.ds((line + core * upper) & (pay.lines - 1), 1)
        high, low = highs_ref[at, :], lows_ref[at, :]
        pool_ref[:, line * 128 : line * 128 + 128] = (high * 128.0 + low).astype(jnp.int32)
        if line < upper:
            high_rows.append(high)
            low_rows.append(low)
    tail = message_ref.shape[0] - half - upper
    zeros = [jnp.zeros((tail, 128), F32)]
    ids = jnp.concatenate(
        [jnp.concatenate(high_rows + zeros, axis=0), jnp.concatenate(low_rows + zeros, axis=0)],
        axis=1,
    )
    message_ref[half:, :] = ids.astype(BF)

    mid_ref[:half, :] = mine_ref[...]
    mid_ref[half:, :] = other_ref[...]
    own = (0.25 * mid_ref[:, :width].astype(F32)).astype(BF)
    send_t = dot(send_ref[...].T, own, NT).astype(BF)
    recv_t = dot(recv_ref[...].T, own, NT).astype(BF)
    away = dot(send_t, hot(ext_ref[...], group_coarse), NN).astype(BF)
    send_t = jnp.concatenate([send_t, away], axis=1)
    edges_forward(src_ref, dst_ref, send_t, recv_t, slope_ref, acc_ref, size)
    mid = (own.astype(F32) + dot(acc_ref[...].astype(BF), node_ref[...], NN)).astype(BF)
    mid_ref[:, :width] = mid
    message_ref[:half, :width] = mid[:half]
    message_ref[:half, width:] = mine_ref[:, width:]


def coarse_backward_kernel(
    size, src_ref, dst_ref, ext_ref, pool_ref, mid_ref, slope_ref, top_ref, send_ref, recv_ref,
    node_ref, *refs,
):
    *others, out_ref, by_src_ref, by_dst_ref, mids_ref = refs
    own_count, width = by_dst_ref.shape
    half = own_count // 2
    mids_ref[:own_count, :] = mid_ref[...]
    rows = [pool_ref[...]]
    for i, ref in enumerate(others):
        mids_ref[own_count + i * half : own_count + i * half + half, :] = ref[:half, :]
        ids = ref[half:, :].astype(F32)
        for line in range(half // 128):
            high, low = ids[line : line + 1, :128], ids[line : line + 1, 128:]
            rows.append((high * 128.0 + low).astype(jnp.int32))
    mids = mids_ref[...]
    own = mid_ref[...].astype(F32)
    pools = hot(jnp.concatenate(rows, axis=1), NCC)
    sums = dot(pools, mids, NN)
    pooled = 0.125 * sums[:, :width]
    grad_top = sums[:, width:]
    weight = top_ref[...]
    slope_in = dot(pooled.astype(BF), weight, NN)
    sigma = sigmoid(slope_in)
    top_out = (pooled + slope_in * sigma).astype(BF)
    inner = (grad_top * (sigma * (1.0 + slope_in * (1.0 - sigma)))).astype(BF)
    grad_pool = 0.125 * (grad_top + dot(inner, weight, NT))
    both = jnp.concatenate([top_out, grad_pool.astype(BF)], axis=1)
    at_node = dot(pools[:, :own_count], both, TN)
    coarse_out = (own[:, :width] + at_node[:, :width]).astype(BF)
    grad = own[:, width:] + at_node[:, width:]
    grad_t = dot(node_ref[...], grad.astype(BF), NT).astype(BF)
    edges_backward(src_ref, dst_ref, grad_t, slope_ref, by_src_ref, by_dst_ref, size)
    by_src = by_src_ref[...]
    away = dot(hot(ext_ref[...], own_count), by_src[own_count:].astype(BF), NN)
    grad = grad + dot((by_src[:own_count] + away).astype(BF), send_ref[...], NT)
    grad = grad + dot(by_dst_ref[...].astype(BF), recv_ref[...], NT)
    out_ref[...] = jnp.concatenate([coarse_out, (0.25 * grad).astype(BF)], axis=1)


def fine_backward_kernel(
    size, slots, src_ref, dst_ref, pool_ref, ext_ref, cot_ref, coarse_ref, slope_ref,
    send_ref, node_ref, at_ref, gpre_ref, sums_ref, odd_ref, even_ref, weight_ref, near_ref,
    far_ref, by_src_ref, all_ref, away_ref,
):
    core = lax.axis_index("dom") & 1
    count, width = cot_ref.shape
    at_node = dot(hot(pool_ref[...], coarse_ref.shape[0]), coarse_ref[...], TN)
    at_ref[...] = at_node
    grad = cot_ref[...].astype(F32) + at_node[:, width:]
    grad_t = dot(node_ref[...], grad.astype(BF), NT).astype(BF)
    edges_backward(src_ref, dst_ref, grad_t, slope_ref, by_src_ref, None, size, gpre_ref)
    by_src = by_src_ref[...].astype(BF)
    sums_ref[...] = by_src[:count]
    away = dot(by_src[count:], send_ref[...], NT).astype(BF)
    pairs = even_ref.shape[0] // slots
    for chip in range(pairs):
        at = 2 * chip * slots
        even_ref[chip * slots : chip * slots + slots, :] = away[at : at + slots]
        odd_ref[chip * slots : chip * slots + slots, :] = away[at + slots : at + 2 * slots]
    halo = 2 * pairs * slots
    rim = near_ref.shape[0]
    away_ref[...] = away[halo:]
    near, far = rim_spots(0, rim, lax.axis_index("group") & 1)
    near_ref[...] = away_ref[near, :]
    far_ref[...] = away_ref[far, :]
    all_ref[...] = dot(ext_ref[...], by_src, TN)
    half = width // 2
    weight_ref[...] = all_ref[pl.ds(pl.multiple_of(core * half, half), half), :].astype(BF)
    there = pl.ds(pl.multiple_of((1 - core) * half, half), half)
    odd_ref[pairs * slots :, :] = all_ref[there, :].astype(BF)


def fine_own_kernel(
    size, dst_ref, gpre_ref, at_ref, sums_ref, cot_ref, upd_ref, send_ref, recv_ref,
    flow_ref, own_ref, by_dst_ref,
):
    count, width = cot_ref.shape
    by_dst_ref[...] = jnp.zeros_like(by_dst_ref)

    def step(i, carry):
        at = pl.ds(pl.multiple_of(i * size, size), size)
        by_dst_ref[...] += dot(hot(dst_ref[:, at], count), gpre_ref[:, at], NT)
        return carry

    lax.fori_loop(0, dst_ref.shape[1] // size, step, 0)
    at_node = at_ref[...]
    flow_ref[...] = (upd_ref[...].astype(F32) + at_node[:, :width]).astype(BF)
    own = cot_ref[...].astype(F32) + at_node[:, width:]
    own = own + dot(sums_ref[...], send_ref[...], NT)
    own_ref[...] = own + dot(by_dst_ref[...].astype(BF), recv_ref[...], NT)


def pack_back_kernel(slots, even_ref, got_ref, weight_ref, *refs):
    *out_refs, half_ref = refs
    chips = len(out_refs) + 1
    half = weight_ref[...].astype(F32) + got_ref[chips * slots :, :].astype(F32)
    half_ref[...] = half.astype(BF)
    for chip, ref in enumerate(out_refs, 1):
        ref[:slots, :] = even_ref[chip * slots : chip * slots + slots, :]
        ref[slots : 2 * slots, :] = got_ref[chip * slots : chip * slots + slots, :]
        ref[2 * slots :, :] = half.astype(BF)


def weight_kernel(skip, half_ref, near_ref, far_ref, *refs):
    *landed, out_ref = refs
    parts = [half_ref[...]] + [ref[skip:, :] for ref in landed]
    out_ref[...] = tree_sum(parts).astype(BF)


def return_kernel(
    send_ref, rim_ref, own_ref, even_ref, got_ref, near_ref, far_ref, *refs
):
    *landed, out_ref, rows_ref = refs
    me = lax.axis_index("dom")
    _, slots = send_ref.shape
    pieces = [even_ref[:slots, :], got_ref[:slots, :]]
    for ref in landed:
        pieces += [ref[:slots, :], ref[slots : 2 * slots, :]]
    for j, piece in enumerate(pieces):
        rows_ref[pl.ds(pl.multiple_of((me ^ j) * slots, slots), slots), :] = piece
    count = own_ref.shape[0]
    total = own_ref[...] + dot(hot(send_row(send_ref), count), rows_ref[...], NN)
    odd_group = lax.axis_index("group") & 1
    near, far = rim_ref[pl.ds(1 - odd_group, 1), :], rim_ref[pl.ds(odd_group, 1), :]
    total = total + dot(hot(near, count), near_ref[...], NN)
    out_ref[...] = total + dot(hot(far, count), far_ref[...], NN)


def join_kernel(mine_ref, other_ref, out_ref):
    core = lax.axis_index("dom") & 1
    half = mine_ref.shape[0]
    out_ref[pl.ds(pl.multiple_of(core * half, half), half), :] = mine_ref[...]
    out_ref[pl.ds(pl.multiple_of((1 - core) * half, half), half), :] = other_ref[...]


def to_xor(value, axis, offset):
    count = lax.axis_size(axis)
    return lax.ppermute(value, axis, [(i, i ^ offset) for i in range(count)])


def step(
    features, cotangent, fine_send, fine_rim, fine_src, fine_dst, fine_pool, coarse_send,
    coarse_src, coarse_dst, coarse_pool, w_send, w_recv, w_node, v_send, v_recv, v_node, w_top,
):
    count, width = features.shape
    doms = lax.axis_size("dom")
    groups = lax.axis_size("group")
    chips = doms // 2
    slots = fine_send.shape[1]
    cslots = coarse_send.shape[1]
    rim = fine_rim.shape[1]
    coarse = coarse_pool.shape[0]
    group_coarse = coarse * doms
    half_coarse = group_coarse // 2
    edges = fine_src.shape[0]
    cedges = coarse_src.shape[0]
    near = [(i, i ^ 1) for i in range(groups)]
    far = [(i, i - 1 + 2 * (i & 1)) for i in range(1, groups - 1)]
    ext_count = count + doms * slots + 2 * rim
    cext_count = group_coarse + doms * doms * cslots
    pay = Payload(cedges, group_coarse, doms)
    assert coarse + doms * cslots <= 256 and doms * cslots <= 128 and width == 128
    src_row, dst_row = fine_src.reshape(1, -1), fine_dst.reshape(1, -1)
    (here,) = call(where_kernel, [((8, 128), jnp.int32)], cost=LONG)
    odd, even, payload, near_rows, far_rows, pool_row = call(
        functools.partial(start_kernel, pay),
        [((chips * slots + pay.rows, width), BF), ((chips * slots, width), BF),
         ((pay.rows, width), BF), ((rim, width), BF), ((rim, width), BF),
         ((1, count), jnp.int32)],
        here, fine_send, fine_rim, coarse_src.reshape(-1, 128), coarse_dst.reshape(-1, 128),
        coarse_pool.reshape(1, -1), coarse_send.T, fine_pool.reshape(1, -1), features,
        scratch=[((doms * slots, width), BF), ((pay.rows, 128), F32)], cost=LONG,
    )
    got = to_xor(odd, "dom", 1)
    messages = call(
        functools.partial(pack_kernel, slots),
        [((2 * slots + 2 * pay.rows, width), BF)] * (chips - 1), even, got, payload,
    )
    landed = [to_xor(message, "dom", 2 * o) for o, message in enumerate(messages, 1)]
    near_rows = lax.ppermute(near_rows, "group", near)
    far_rows = lax.ppermute(far_rows, "group", far)

    size = chunk_of(edges, (2048 << 10) // ext_count)
    (known,) = call(
        functools.partial(fine_local_kernel, size), [((width, edges), F32)],
        src_row, dst_row, features, w_send, w_recv, cost=4 * width * count * edges,
    )
    updated, mine, other, slope, extended, src_row = call(
        functools.partial(fine_forward_kernel, min(2 * size, edges), slots),
        [((count, width), BF), ((half_coarse, 2 * width), BF), ((half_coarse, 2 * width), BF),
         ((width, edges), BF), ((ext_count, width), BF), ((1, edges), jnp.int32)],
        src_row, dst_row, pool_row, features, even, got, near_rows, far_rows,
        cotangent, w_send, known, w_node, *landed,
        scratch=[((count, width), F32), ((1, edges), jnp.int32)], extra=10 << 20,
    )
    half_sum = [((half_coarse, 2 * width), BF)]
    (mine,) = call(add_kernel, half_sum, mine, to_xor(other, "dom", 1))
    parts = [to_xor(mine, "dom", 2 * o) for o in range(1, chips)]
    (mine,) = call(add_kernel, half_sum, mine, *parts)
    other = to_xor(mine, "dom", 1)

    csize = chunk_of(cedges * doms, (1 << 20) // cext_count)
    extra = 3 * cext_count * 2 * max(csize, group_coarse)
    tail = -(-(pay.lines // 2) // 16) * 16
    message, mid, cslope, csrc_row, cdst_row, cext_row, pools = call(
        functools.partial(coarse_forward_kernel, pay, csize, coarse),
        [((half_coarse + tail, 2 * width), BF), ((group_coarse, 2 * width), BF),
         ((width, cedges * doms), BF), ((1, cedges * doms), jnp.int32),
         ((1, cedges * doms), jnp.int32), ((1, doms * doms * cslots), jnp.int32),
         ((1, group_coarse), jnp.int32)],
        mine, other, v_send, v_recv, v_node, payload, got, *landed,
        scratch=[((group_coarse, width), F32), ((doms, 128), F32), ((pay.lines, 128), F32),
                 ((pay.lines, 128), F32)],
        extra=extra,
    )
    others = [to_xor(message, "group", o) for o in range(1, groups)]
    others += [to_xor(part, "dom", 1) for part in others]
    (back,) = call(
        functools.partial(coarse_backward_kernel, csize),
        [((group_coarse, 2 * width), BF)],
        csrc_row, cdst_row, cext_row, pools, mid, cslope, w_top, v_send, v_recv, v_node, *others,
        scratch=[((cext_count, width), F32), ((group_coarse, width), F32),
                 ((groups * group_coarse, 2 * width), BF)],
        extra=extra,
    )

    half = width // 2
    at_node, gpre, sums, odd, even, weight, near_rows, far_rows = call(
        functools.partial(fine_backward_kernel, size, slots),
        [((count, 2 * width), F32), ((width, edges), BF), ((count, width), BF),
         ((chips * slots + half, width), BF), ((chips * slots, width), BF), ((half, width), BF),
         ((rim, width), BF), ((rim, width), BF)],
        src_row, dst_row, pool_row, extended, cotangent, back, slope, w_send, w_node,
        scratch=[((ext_count, width), F32), ((width, width), F32), ((2 * rim, width), BF)],
    )
    flow, own = call(
        functools.partial(fine_own_kernel, size),
        [((count, width), BF), ((count, width), F32)],
        dst_row, gpre, at_node, sums, cotangent, updated, w_send, w_recv,
        scratch=[((count, width), F32)], cost=2 * width * count * edges,
    )

    got = to_xor(odd, "dom", 1)
    *messages, weight = call(
        functools.partial(pack_back_kernel, slots),
        [((2 * slots + half, width), BF)] * (chips - 1) + [((half, width), BF)],
        even, got, weight,
    )
    landed = []
    for o, message in enumerate(messages, 1):
        landed.append(to_xor(message, "dom", 2 * o))
    near_rows = lax.ppermute(near_rows, "group", near)
    far_rows = lax.ppermute(far_rows, "group", far)
    (weight,) = call(
        functools.partial(weight_kernel, 2 * slots), [((half, width), BF)], weight, near_rows,
        far_rows, *landed,
    )
    parts = []
    for o in range(1, groups):
        parts.append(to_xor(weight, "group", o))
    (grad_x,) = call(
        return_kernel, [((count, width), F32)],
        fine_send, fine_rim, own, even, got, near_rows, far_rows, *landed,
        scratch=[((doms * slots, width), BF)], cost=width * count * edges,
    )
    (weight,) = call(add_kernel, [((half, width), F32)], weight, *parts)
    (grad_send,) = call(
        join_kernel, [((width, width), F32)], weight, to_xor(weight, "dom", 1)
    )
    return flow, grad_x, grad_send


def solution(mesh):
    rows = P(("group", "dom"), None)
    line = P(("group", "dom"))
    placed = (rows, rows, rows, rows, line, line, line, rows, line, line, line) + (P(),) * 7
    return jax.shard_map(
        step, mesh=mesh, in_specs=placed, out_specs=(rows, rows, P()), check_vma=False
    )
```
